16 devices in a mesh: dp: 2 (over y, z), sp: 8 (over x, core).
Axes of the slice: x: 4, y: 2, z: 1, core: 2. Of those that a mesh axis runs over, the one named last changes fastest.
The devices are a block of a 4x4x8 slice.
Arguments:
- resid_x: bfloat16 [32, 1024, 2048], P('dp', 'sp'), parts along dimension 0
- positions: int32 [32, 1024], P('dp', 'sp'), parts along dimension 0
- w_query: bfloat16 [2048, 2048], replicated
- w_key: bfloat16 [2048, 2048], replicated
- w_value: bfloat16 [2048, 2048], replicated
- w_out: bfloat16 [2048, 2048], replicated
- gain_q: bfloat16 [2048], replicated
- gain_k: bfloat16 [2048], replicated
- gain_out: bfloat16 [2048], replicated
Outputs:
- output: bfloat16 [32, 1024, 2048], P('dp', 'sp'), parts along dimension 0
There are 2 independent parts. The reference program is written for one: setup_inputs(seed, part) draws one part's arguments, and reference() takes and returns one part's arrays. A program takes and returns all parts, laid end to end along the dimension named above; an argument that names none is the same for every part.
All inputs are finite; a program needn't handle non-finite values.
Results may differ from the reference program's by a relative error of at most 0.0178911.
Values are sent between devices in bfloat16 or wider.
A program may use at most 768 MiB of HBM per device.

```python
import jax
import jax.numpy as jnp
from jax import lax

BATCH = 16
SEQ = 1024
D_MODEL = 2048
HEADS = 16
HEAD_DIM = 128
DOC_LEN = 512
QUERY_BLOCKS = 8
ROPE_THETA = 500000.0
NORM_EPS = 1e-6
SCALE = HEAD_DIM ** -0.5


def setup_inputs(seed: int = 0, part: int = 0) -> dict:
    base_key = jax.random.key(seed)
    shared_keys = jax.random.split(base_key, 8)
    part_keys = jax.random.split(jax.random.fold_in(shared_keys[7], part), 2)
    resid_x = jax.random.normal(part_keys[0], (BATCH, SEQ, D_MODEL), jnp.float32).astype(jnp.bfloat16)
    token_idx = jnp.arange(SEQ, dtype=jnp.int32)[None, :]
    starts = jax.random.randint(part_keys[1], (BATCH, SEQ), 0, DOC_LEN) == 0
    starts = jnp.logical_or(starts, token_idx == 0)
    last_start = lax.cummax(jnp.where(starts, token_idx, 0), axis=1)
    positions = (token_idx - last_start).astype(jnp.int32)
    w_scale = D_MODEL ** -0.5
    matrices = [(jax.random.normal(shared_keys[w_idx], (D_MODEL, D_MODEL), jnp.float32) * w_scale).astype(jnp.bfloat16) for w_idx in range(4)]
    gains = [(0.5 + jax.random.normal(shared_keys[4 + g_idx], (D_MODEL,), jnp.float32)).astype(jnp.bfloat16) for g_idx in range(3)]
    return {'resid_x': resid_x, 'positions': positions, 'w_query': matrices[0], 'w_key': matrices[1], 'w_value': matrices[2], 'w_out': matrices[3], 'gain_q': gains[0], 'gain_k': gains[1], 'gain_out': gains[2]}


def rope_tables(pos_ids):
    inv_freq = 1.0 / (ROPE_THETA ** (jnp.arange(0, HEAD_DIM, 2, dtype=jnp.float32) / HEAD_DIM))
    angles = pos_ids.astype(jnp.float32)[..., None] * inv_freq
    return jnp.cos(angles), jnp.sin(angles)


def apply_rope(heads_f32, cos_t, sin_t):
    half = HEAD_DIM // 2
    cos_b = cos_t[:, :, None, :]
    sin_b = sin_t[:, :, None, :]
    first = heads_f32[..., :half]
    second = heads_f32[..., half:]
    return jnp.concatenate([first * cos_b - second * sin_b, second * cos_b + first * sin_b], axis=-1)


def rms_scale(vals_f32, gain):
    mean_sq = jnp.mean(vals_f32 * vals_f32, axis=-1, keepdims=True)
    return vals_f32 * lax.rsqrt(mean_sq + NORM_EPS) * gain.astype(jnp.float32)


def norm_rope(x_rows, weight, gain, cos_t, sin_t):
    proj = jnp.dot(x_rows, weight, preferred_element_type=jnp.float32).astype(jnp.bfloat16).astype(jnp.float32)
    normed = rms_scale(proj, gain).reshape(BATCH, SEQ, HEADS, HEAD_DIM)
    return apply_rope(normed, cos_t, sin_t).astype(jnp.bfloat16)


def head_attention(operands):
    q_head, k_head, v_head = operands
    block = SEQ // QUERY_BLOCKS
    q_blocks = q_head.reshape(BATCH, QUERY_BLOCKS, block, HEAD_DIM).transpose(1, 0, 2, 3)
    k_f32 = k_head.astype(jnp.float32)
    v_f32 = v_head.astype(jnp.float32)
    key_idx = jnp.arange(SEQ)

    def one_block(blk_ops):
        q_blk, blk_idx = blk_ops
        scores = jnp.einsum('bqd,bkd->bqk', q_blk.astype(jnp.float32), k_f32) * SCALE
        q_idx = blk_idx * block + jnp.arange(block)
        mask = key_idx[None, :] <= q_idx[:, None]
        scores = jnp.where(mask[None], scores, -1e30)
        probs = jax.nn.softmax(scores, axis=-1).astype(jnp.bfloat16).astype(jnp.float32)
        return jnp.einsum('bqk,bkd->bqd', probs, v_f32).astype(jnp.bfloat16)

    out_blocks = lax.map(one_block, (q_blocks, jnp.arange(QUERY_BLOCKS)))
    return out_blocks.transpose(1, 0, 2, 3).reshape(BATCH, SEQ, HEAD_DIM)


def reference(resid_x, positions, w_query, w_key, w_value, w_out, gain_q, gain_k, gain_out):
    cos_t, sin_t = rope_tables(positions)
    x_rows = resid_x.reshape(BATCH * SEQ, D_MODEL)
    q_all = norm_rope(x_rows, w_query, gain_q, cos_t, sin_t)
    k_all = norm_rope(x_rows, w_key, gain_k, cos_t, sin_t)
    v_all = jnp.dot(x_rows, w_value, preferred_element_type=jnp.float32).astype(jnp.bfloat16).reshape(BATCH, SEQ, HEADS, HEAD_DIM)
    per_head = lax.map(head_attention, (q_all.transpose(2, 0, 1, 3), k_all.transpose(2, 0, 1, 3), v_all.transpose(2, 0, 1, 3)))
    attn_rows = per_head.transpose(1, 2, 0, 3).reshape(BATCH * SEQ, D_MODEL)
    attn_out = jnp.dot(attn_rows, w_out, preferred_element_type=jnp.float32).astype(jnp.bfloat16).astype(jnp.float32)
    y_rows = x_rows.astype(jnp.float32) + rms_scale(attn_out, gain_out)
    return y_rows.astype(jnp.bfloat16).reshape(BATCH, SEQ, D_MODEL)
```

```python
import functools
import math

import jax
import jax.numpy as jnp
import numpy as np
from jax import lax
from jax.experimental import pallas as pl
from jax.experimental.pallas import tpu as pltpu
from jax.sharding import PartitionSpec as P

HEAD_DIM = 128
ROPE_THETA = 500000.0
NORM_EPS = 1e-6
SCALE = HEAD_DIM ** -0.5
EXP2_SCALE = SCALE * math.log2(math.e)
CORES = 2
MESH = pl.DeviceIdType.MESH
VMEM_LIMIT = 67043328
COMM = True

PIO2 = (1.5703125, 4.837512969970703125e-4, 7.54978995489188216e-8)


def cos_sin_rows(angles, lane_low):
    quad = jnp.floor(angles * (2.0 / math.pi) + 0.5)
    r = angles - quad * PIO2[0]
    r = r - quad * PIO2[1]
    r = r - quad * PIO2[2]
    r2 = r * r
    sin_r = r + r * r2 * (-1.6666654611e-1 + r2 * (8.3321608736e-3 + r2 * -1.9515295891e-4))
    cos_r = 1.0 - 0.5 * r2 + r2 * r2 * (4.166664568298827e-2 + r2 * (-1.388731625493765e-3 + r2 * 2.443315711809948e-5))
    quad = jnp.where(lane_low, quad, quad + 3.0)
    quad = quad - 4.0 * jnp.floor(quad * 0.25)
    odd = jnp.logical_or(quad == 1.0, quad == 3.0)
    val = jnp.where(odd, sin_r, cos_r)
    neg = jnp.logical_or(quad == 1.0, quad == 2.0)
    return jnp.where(neg, -val, val)


def block_kernel(n, x_hbm, pos_hbm, freq_ref, gq_ref, gk_ref, ga_ref, wq_hbm, wk_hbm, wv_hbm, wo_hbm, y_hbm,
                 wq, wk, wv, wo, xb, q, k, v, a_buf, posb, cosb, sinb,
                 w_sem, p_send, p_recv, x_send, x_recv, y_send, y_recv):
    batch, t_loc, width = x_hbm.shape
    n_seq = batch // n
    chips = n // CORES
    rows_blk = CORES * t_loc
    heads = width // HEAD_DIM
    me = lax.axis_index("sp")
    chip = me // CORES
    core = lax.rem(me, CORES)

    def peer(hop, swap):
        other = core if swap == 0 else 1 - core
        return lax.rem(chip + hop, chips) * CORES + other

    peers = [(0, 1)] + [(h, w) for w in range(CORES) for h in (1, chips - 1)] + [(h, w) for h in range(2, chips - 1) for w in range(CORES)]

    w_copies = []
    for idx, (src, dst) in enumerate(((wq_hbm, wq), (wk_hbm, wk), (wv_hbm, wv), (wo_hbm, wo))):
        cp = pltpu.make_async_copy(src, dst, w_sem.at[idx])
        w_copies.append(cp)
    pos_own = pltpu.make_async_copy(pos_hbm, posb.at[me], p_recv.at[0])
    pos_own.start()
    own = [pltpu.make_async_copy(x_hbm.at[me * n_seq + s], xb.at[s, pl.ds(pl.multiple_of(me * t_loc, t_loc), t_loc)], x_recv.at[s, 0]) for s in range(n_seq)]
    for cp in own:
        cp.start()
    for cp in w_copies:
        cp.start()

    sends = []
    if COMM:
        barrier = pltpu.get_barrier_semaphore()
        for hop, swap in peers:
            pl.semaphore_signal(barrier, inc=1, device_id={"sp": peer(hop, swap)}, device_id_type=MESH)
        pl.semaphore_wait(barrier, n - 1)
        my_rows = pl.ds(pl.multiple_of(me * t_loc, t_loc), t_loc)
        for hop, swap in peers:
            tag = hop * CORES + swap
            cp = pltpu.make_async_remote_copy(src_ref=pos_hbm, dst_ref=posb.at[me], send_sem=p_send.at[tag], recv_sem=p_recv.at[tag],
                                              device_id={"sp": peer(hop, swap)}, device_id_type=MESH)
            cp.start()
            sends.append(cp)
        for s in range(n_seq):
            for hop, swap in peers:
                tag = hop * CORES + swap
                to = peer(hop, swap)
                cp = pltpu.make_async_remote_copy(src_ref=x_hbm.at[to * n_seq + s], dst_ref=xb.at[s, my_rows],
                                                  send_sem=x_send.at[s, tag], recv_sem=x_recv.at[s, tag],
                                                  device_id={"sp": to}, device_id_type=MESH)
                cp.start()
                sends.append(cp)

    pos_own.wait()
    if COMM:
        for tag in range(1, n):
            pltpu.make_async_copy(pos_hbm, posb.at[0], p_recv.at[tag]).wait()
    for cp in w_copies:
        cp.wait()

    lane = lax.broadcasted_iota(jnp.int32, (t_loc, HEAD_DIM), 1)
    row = lax.broadcasted_iota(jnp.int32, (t_loc, HEAD_DIM), 0)
    lane_low = lane < HEAD_DIM // 2
    eye = lane == row
    tri = lane <= row

    def tables(s):
        def one(j, _):
            pos_row = posb[j, pl.ds(me * n_seq + s, 1), :].astype(jnp.float32)
            pos_col = jnp.sum(jnp.where(eye, jnp.broadcast_to(pos_row, (t_loc, HEAD_DIM)), 0.0), axis=1, keepdims=True)
            both = cos_sin_rows(pos_col * freq_ref[...], lane_low)
            turned = pltpu.roll(both, HEAD_DIM // 2, 1)
            at = pl.ds(pl.multiple_of(j * t_loc, t_loc), t_loc)
            cosb[at, :] = jnp.where(lane_low, both, turned)
            sinb[at, :] = jnp.where(lane_low, -turned, both)
            return 0
        lax.fori_loop(0, n, one, 0)

    NT = 256
    RC = 32

    def matmul(lhs, w, put):
        def one(j, _):
            at = pl.ds(pl.multiple_of(j * NT, NT), NT)
            put(at, jnp.dot(lhs(), w[:, at], preferred_element_type=jnp.float32).astype(jnp.bfloat16))
            return 0
        lax.fori_loop(0, width // NT, one, 0)

    def sum_sq(load):
        total = None
        for h in range(heads):
            t = load(h)
            total = t * t if total is None else total + t * t
        return lax.rsqrt(jnp.sum(total, axis=1, keepdims=True) * (1.0 / width) + NORM_EPS)

    def norm_rope(buf, base, gain):
        def one(i, _):
            at = pl.ds(pl.multiple_of(base + i * RC, RC), RC)
            load = lambda h: buf[at, h * HEAD_DIM:(h + 1) * HEAD_DIM].astype(jnp.float32)
            rs = sum_sq(load)
            cos_t = cosb[at, :]
            sin_t = sinb[at, :]
            for h in range(heads):
                cols = slice(h * HEAD_DIM, (h + 1) * HEAD_DIM)
                t = load(h) * rs * gain[:, cols].astype(jnp.float32)
                buf[at, cols] = (t * cos_t + pltpu.roll(t, HEAD_DIM // 2, 1) * sin_t).astype(jnp.bfloat16)
            return 0
        lax.fori_loop(0, rows_blk // RC, one, 0)

    HU = 2

    def attend(blk):
        for half in range(CORES):
            r0 = blk * rows_blk + half * t_loc
            kv = r0 + t_loc

            def some_heads(i, _, r0=r0, kv=kv):
                for u in range(HU):
                    cols = pl.ds(pl.multiple_of((i * HU + u) * HEAD_DIM, HEAD_DIM), HEAD_DIM)
                    q_h = q[r0:r0 + t_loc, cols]
                    s = lax.dot_general(q_h, k[0:kv, cols], (((1,), (1,)), ((), ())), preferred_element_type=jnp.float32)
                    last = jnp.where(tri, s[:, r0:], -1e30)
                    s = last if r0 == 0 else jnp.concatenate([s[:, :r0], last], axis=1)
                    m = jnp.max(s, axis=1, keepdims=True)
                    p = jnp.exp2((s - m) * EXP2_SCALE)
                    p = (p * (1.0 / jnp.sum(p, axis=1, keepdims=True))).astype(jnp.bfloat16)
                    q[r0:r0 + t_loc, cols] = jnp.dot(p, v[0:kv, cols], preferred_element_type=jnp.float32).astype(jnp.bfloat16)
                return 0
            lax.fori_loop(0, heads // HU, some_heads, 0)

    def hop_of(b, order):
        hop = order[-1]
        for i in range(len(order) - 1):
            hop = jnp.where(b == i, order[i], hop)
        return hop

    near = [h for h in (1, chips - 1)] + list(range(2, chips - 1))

    def sequence(s, _):
        tables(s)

        def project(b, _):
            hop = hop_of(b, [0] + near)
            c = lax.rem(chip + hop, chips)
            tag = lax.rem(chips - hop, chips) * CORES
            base = pl.multiple_of(c * rows_blk, rows_blk)
            rows = pl.ds(base, rows_blk)

            @pl.when(hop == 0)
            def _():
                pltpu.make_async_copy(x_hbm.at[0], xb.at[s, pl.ds(0, t_loc)], x_recv.at[s, 0]).wait()
                if COMM:
                    pltpu.make_async_copy(x_hbm.at[0], xb.at[s, pl.ds(0, t_loc)], x_recv.at[s, 1]).wait()

            if COMM:
                @pl.when(hop != 0)
                def _():
                    for w in range(CORES):
                        pltpu.make_async_copy(x_hbm.at[0], xb.at[s, pl.ds(0, t_loc)], x_recv.at[s, tag + w]).wait()

            lhs = lambda: xb[s, rows, :]

            def putter(buf):
                def put(at, val):
                    buf[rows, at] = val
                return put
            matmul(lhs, wq, putter(q))
            norm_rope(q, base, gq_ref)
            matmul(lhs, wk, putter(k))
            norm_rope(k, base, gk_ref)
            matmul(lhs, wv, putter(v))
            return 0
        lax.fori_loop(0, chips, project, 0)

        def finish(b, _):
            hop = hop_of(b, near + [0])
            c = lax.rem(chip + hop, chips)
            base = pl.multiple_of(c * rows_blk, rows_blk)
            rows = pl.ds(base, rows_blk)
            for blk in range(chips):
                @pl.when(c == blk)
                def _():
                    attend(blk)

            def put(at, val):
                a_buf[:, at] = val
            matmul(lambda: q[rows, :], wo, put)

            def out_rows(i, _):
                at = pl.ds(pl.multiple_of(i * RC, RC), RC)
                xat = pl.ds(pl.multiple_of(base + i * RC, RC), RC)
                load = lambda h: a_buf[at, h * HEAD_DIM:(h + 1) * HEAD_DIM].astype(jnp.float32)
                rs = sum_sq(load)
                for h in range(heads):
                    cols = slice(h * HEAD_DIM, (h + 1) * HEAD_DIM)
                    res = xb[s, xat, cols].astype(jnp.float32)
                    xb[s, xat, cols] = (res + load(h) * rs * ga_ref[:, cols].astype(jnp.float32)).astype(jnp.bfloat16)
                return 0
            lax.fori_loop(0, rows_blk // RC, out_rows, 0)

            def send(w):
                to = c * CORES + (core if w == 0 else 1 - core)
                src = xb.at[s, pl.ds(pl.multiple_of(to * t_loc, t_loc), t_loc)]
                pltpu.make_async_remote_copy(src_ref=src, dst_ref=y_hbm.at[me * n_seq + s], send_sem=y_send.at[s, hop * CORES + w],
                                             recv_sem=y_recv.at[s, hop * CORES + w], device_id={"sp": to}, device_id_type=MESH).start()

            @pl.when(hop == 0)
            def _():
                src = xb.at[s, pl.ds(pl.multiple_of(me * t_loc, t_loc), t_loc)]
                pltpu.make_async_copy(src, y_hbm.at[me * n_seq + s], y_recv.at[s, 0]).start()
                if COMM:
                    send(1)

            if COMM:
                @pl.when(hop != 0)
                def _():
                    send(0)
                    send(1)
            return 0
        lax.fori_loop(0, chips, finish, 0)
        return 0

    lax.fori_loop(0, n_seq, sequence, 0)

    for s in range(n_seq):
        for tag in range(n if COMM else 1):
            pltpu.make_async_copy(xb.at[s, pl.ds(0, t_loc)], y_hbm.at[0], y_recv.at[s, tag]).wait()
    if COMM:
        for s in range(n_seq):
            for tag in range(1, n):
                pltpu.make_async_copy(xb.at[s, pl.ds(0, t_loc)], y_hbm.at[0], y_send.at[s, tag]).wait()
        for cp in sends:
            cp.wait_send()


def solution(mesh):
    n = mesh.shape["sp"]

    def local_block(x_loc, pos_loc, w_query, w_key, w_value, w_out, gain_q, gain_k, gain_out):
        batch, t_loc, width = x_loc.shape
        n_seq = batch // n
        inv_freq = 1.0 / (ROPE_THETA ** (np.arange(0, HEAD_DIM, 2, dtype=np.float32) / HEAD_DIM))
        freq = jnp.asarray(np.concatenate([inv_freq, inv_freq]).astype(np.float32)[None, :])
        hbm = pl.BlockSpec(memory_space=pl.ANY)
        vmem = pl.BlockSpec(memory_space=pltpu.VMEM)
        seq = n * t_loc
        bf16 = jnp.bfloat16
        return pl.pallas_call(
            functools.partial(block_kernel, n),
            out_shape=jax.ShapeDtypeStruct(x_loc.shape, bf16),
            in_specs=[hbm, hbm, vmem, vmem, vmem, vmem, hbm, hbm, hbm, hbm],
            out_specs=hbm,
            scratch_shapes=[
                pltpu.VMEM((width, width), bf16), pltpu.VMEM((width, width), bf16), pltpu.VMEM((width, width), bf16), pltpu.VMEM((width, width), bf16),
                pltpu.VMEM((n_seq, seq, width), bf16),
                pltpu.VMEM((seq, width), bf16), pltpu.VMEM((seq, width), bf16), pltpu.VMEM((seq, width), bf16),
                pltpu.VMEM((CORES * t_loc, width), bf16),
                pltpu.VMEM((n, batch, t_loc), jnp.int32),
                pltpu.VMEM((seq, HEAD_DIM), jnp.float32), pltpu.VMEM((seq, HEAD_DIM), jnp.float32),
                pltpu.SemaphoreType.DMA((4,)),
                pltpu.SemaphoreType.DMA((n,)), pltpu.SemaphoreType.DMA((n,)),
                pltpu.SemaphoreType.DMA((n_seq, n)), pltpu.SemaphoreType.DMA((n_seq, n)),
                pltpu.SemaphoreType.DMA((n_seq, n)), pltpu.SemaphoreType.DMA((n_seq, n)),
            ],
            compiler_params=pltpu.CompilerParams(**({"collective_id": 0} if COMM else {}), has_side_effects=True, vmem_limit_bytes=VMEM_LIMIT),
            name="attention_block",
        )(x_loc, pos_loc, freq, gain_q[None, :], gain_k[None, :], gain_out[None, :], w_query, w_key, w_value, w_out)

    tok_spec = P("dp", "sp", None)
    return jax.shard_map(local_block, mesh=mesh, in_specs=(tok_spec, P("dp", "sp"), P(), P(), P(), P(), P(), P(), P()), out_specs=tok_spec, check_vma=False)
```

```python
import functools
import math

import jax
import jax.numpy as jnp
import numpy as np
from jax import lax
from jax.experimental import pallas as pl
from jax.experimental.pallas import tpu as pltpu
from jax.sharding import PartitionSpec as P

HEAD_DIM = 128
ROPE_THETA = 500000.0
NORM_EPS = 1e-6
SCALE = HEAD_DIM ** -0.5
EXP2_SCALE = SCALE * math.log2(math.e)
CORES = 2
MESH = pl.DeviceIdType.MESH
VMEM_LIMIT = 67043328
NT = 1024
RG = 32

PIO2 = (1.5703125, 4.837512969970703125e-4, 7.54978995489188216e-8)


def cos_sin_rows(angles, lane_low):
    quad = jnp.floor(angles * (2.0 / math.pi) + 0.5)
    r = angles - quad * PIO2[0]
    r = r - quad * PIO2[1]
    r = r - quad * PIO2[2]
    r2 = r * r
    sin_r = r + r * r2 * (-1.6666654611e-1 + r2 * (8.3321608736e-3 + r2 * -1.9515295891e-4))
    cos_r = 1.0 - 0.5 * r2 + r2 * r2 * (4.166664568298827e-2 + r2 * (-1.388731625493765e-3 + r2 * 2.443315711809948e-5))
    quad = jnp.where(lane_low, quad, quad + 3.0)
    quad = quad - 4.0 * jnp.floor(quad * 0.25)
    odd = jnp.logical_or(quad == 1.0, quad == 3.0)
    val = jnp.where(odd, sin_r, cos_r)
    neg = jnp.logical_or(quad == 1.0, quad == 2.0)
    return jnp.where(neg, -val, val)


def block_kernel(n, x_hbm, pos_hbm, freq_ref, gains_ref, wq_hbm, wk_hbm, wv_hbm, wo_hbm, y_hbm,
                 wq, wk, wv, wo, xb, q, k, v, a_buf, s_buf, p_buf, posb, cosb, sinb,
                 w_sem, p_send, p_recv, x_send, x_recv, y_send, y_recv):
    batch, t_loc, width = x_hbm.shape
    n_seq = batch // n
    chips = n // CORES
    rows_blk = CORES * t_loc
    heads = width // HEAD_DIM
    me = lax.axis_index("sp")
    chip = me // CORES
    core = lax.rem(me, CORES)

    def peer(hop, swap):
        other = core if swap == 0 else 1 - core
        return lax.rem(chip + hop, chips) * CORES + other

    peers = [(0, 1)] + [(h, w) for w in range(CORES) for h in (1, chips - 1)] + [(h, w) for h in range(2, chips - 1) for w in range(CORES)]

    w_copies = []
    for idx, (src, dst) in enumerate(((wq_hbm, wq), (wk_hbm, wk), (wv_hbm, wv), (wo_hbm, wo))):
        cp = pltpu.make_async_copy(src, dst, w_sem.at[idx])
        w_copies.append(cp)
    pos_own = pltpu.make_async_copy(pos_hbm, posb.at[me], p_recv.at[0])
    pos_own.start()
    own = [pltpu.make_async_copy(x_hbm.at[me * n_seq + s], xb.at[s, pl.ds(pl.multiple_of(me * t_loc, t_loc), t_loc)], x_recv.at[s, 0]) for s in range(n_seq)]
    for cp in own:
        cp.start()
    for cp in w_copies:
        cp.start()

    sends = []
    barrier = pltpu.get_barrier_semaphore()
    for hop, swap in peers:
        pl.semaphore_signal(barrier, inc=1, device_id={"sp": peer(hop, swap)}, device_id_type=MESH)
    pl.semaphore_wait(barrier, n - 1)
    my_rows = pl.ds(pl.multiple_of(me * t_loc, t_loc), t_loc)
    for hop, swap in peers:
        tag = hop * CORES + swap
        cp = pltpu.make_async_remote_copy(src_ref=pos_hbm, dst_ref=posb.at[me], send_sem=p_send.at[tag], recv_sem=p_recv.at[tag],
                                          device_id={"sp": peer(hop, swap)}, device_id_type=MESH)
        cp.start()
        sends.append(cp)
    for s in range(n_seq):
        for hop, swap in peers:
            tag = hop * CORES + swap
            to = peer(hop, swap)
            cp = pltpu.make_async_remote_copy(src_ref=x_hbm.at[to * n_seq + s], dst_ref=xb.at[s, my_rows],
                                              send_sem=x_send.at[s, tag], recv_sem=x_recv.at[s, tag],
                                              device_id={"sp": to}, device_id_type=MESH)
            cp.start()
            sends.append(cp)

    pos_own.wait()
    for tag in range(1, n):
        pltpu.make_async_copy(pos_hbm, posb.at[0], p_recv.at[tag]).wait()

    lane = lax.broadcasted_iota(jnp.int32, (t_loc, HEAD_DIM), 1)
    row = lax.broadcasted_iota(jnp.int32, (t_loc, HEAD_DIM), 0)
    lane_low = lane < HEAD_DIM // 2
    eye = lane == row

    def tables(s):
        def one(j, _):
            pos_row = posb[j, pl.ds(me * n_seq + s, 1), :].astype(jnp.float32)
            pos_col = jnp.sum(jnp.where(eye, jnp.broadcast_to(pos_row, (t_loc, HEAD_DIM)), 0.0), axis=1, keepdims=True)
            both = cos_sin_rows(pos_col * freq_ref[...], lane_low)
            turned = pltpu.roll(both, HEAD_DIM // 2, 1)
            at = pl.ds(pl.multiple_of(j * t_loc, t_loc), t_loc)
            cosb[at, :] = jnp.where(lane_low, both, turned)
            sinb[at, :] = jnp.where(lane_low, -turned, both)
            return 0
        lax.fori_loop(0, n, one, 0)

    RC = 32
    n_iter = width // NT
    side_rows = rows_blk // n_iter

    def matmul(lhs, w, put, side=None):
        def one(j, _):
            at = pl.ds(pl.multiple_of(j * NT, NT), NT)
            put(at, jnp.dot(lhs(), w[:, at], preferred_element_type=jnp.float32).astype(jnp.bfloat16))
            if side is not None:
                for i in range(side_rows // RC):
                    side(j * (side_rows // RC) + i)
            return 0
        lax.fori_loop(0, n_iter, one, 0)

    def sum_sq(load):
        total = None
        for h in range(heads):
            t = load(h)
            total = t * t if total is None else total + t * t
        return lax.rsqrt(jnp.sum(total, axis=1, keepdims=True) * (1.0 / width) + NORM_EPS)

    def norm_rope(buf, base, gain):
        def one(i):
            at = pl.ds(pl.multiple_of(base + i * RC, RC), RC)
            load = lambda h: buf[at, h * HEAD_DIM:(h + 1) * HEAD_DIM].astype(jnp.float32)
            rs = sum_sq(load)
            cos_t = cosb[at, :]
            sin_t = sinb[at, :]
            for h in range(heads):
                cols = slice(h * HEAD_DIM, (h + 1) * HEAD_DIM)
                t = load(h) * rs * gains_ref[gain:gain + 1, cols].astype(jnp.float32)
                buf[at, cols] = (t * cos_t + pltpu.roll(t, HEAD_DIM // 2, 1) * sin_t).astype(jnp.bfloat16)
        return one

    def attend(blk):
        r0 = blk * rows_blk
        kv = r0 + rows_blk
        tri = lax.broadcasted_iota(jnp.int32, (RG, rows_blk), 1) - lax.broadcasted_iota(jnp.int32, (RG, rows_blk), 0)

        def cols_of(h):
            if isinstance(h, int):
                return slice(h * HEAD_DIM, (h + 1) * HEAD_DIM)
            return pl.ds(pl.multiple_of(h * HEAD_DIM, HEAD_DIM), HEAD_DIM)

        def scores(h, slot):
            cols = cols_of(h)
            s_buf[slot, :, 0:kv] = lax.dot_general(q[r0:kv, cols], k[0:kv, cols], (((1,), (1,)), ((), ())), preferred_element_type=jnp.float32)

        def soft(slot):
            for g in range(rows_blk // RG):
                s = s_buf[slot, g * RG:(g + 1) * RG, 0:kv]
                last = jnp.where(tri <= g * RG, s[:, r0:], -1e30)
                s = last if r0 == 0 else jnp.concatenate([s[:, :r0], last], axis=1)
                m = jnp.max(s, axis=1, keepdims=True)
                p = jnp.exp2((s - m) * EXP2_SCALE)
                p_buf[slot, g * RG:(g + 1) * RG, 0:kv] = (p * (1.0 / jnp.sum(p, axis=1, keepdims=True))).astype(jnp.bfloat16)

        def mix(h, slot):
            cols = cols_of(h)
            q[r0:kv, cols] = jnp.dot(p_buf[slot, :, 0:kv], v[0:kv, cols], preferred_element_type=jnp.float32).astype(jnp.bfloat16)

        scores(0, 0)
        scores(1, 1)
        soft(0)

        def pair(i, _):
            for u in range(2):
                h = 2 + 2 * i + u
                scores(h, u)
                soft(1 - u)
                mix(h - 2, u)
            return 0
        lax.fori_loop(0, heads // 2 - 1, pair, 0)
        soft(1)
        mix(heads - 2, 0)
        mix(heads - 1, 1)

    def hop_of(b, order):
        hop = order[-1]
        for i in range(len(order) - 1):
            hop = jnp.where(b == i, order[i], hop)
        return hop

    near = [h for h in (1, chips - 1)] + list(range(2, chips - 1))
    far = near[2:] + near[:2]

    def sequence(s, _):
        tables(s)

        def project(b, _):
            hop = hop_of(b, [0] + near)
            c = lax.rem(chip + hop, chips)
            tag = lax.rem(chips - hop, chips) * CORES
            base = pl.multiple_of(c * rows_blk, rows_blk)
            rows = pl.ds(base, rows_blk)

            @pl.when(hop == 0)
            def _():
                pltpu.make_async_copy(x_hbm.at[0], xb.at[s, pl.ds(0, t_loc)], x_recv.at[s, 0]).wait()
                pltpu.make_async_copy(x_hbm.at[0], xb.at[s, pl.ds(0, t_loc)], x_recv.at[s, 1]).wait()

            @pl.when(hop != 0)
            def _():
                for w in range(CORES):
                    pltpu.make_async_copy(x_hbm.at[0], xb.at[s, pl.ds(0, t_loc)], x_recv.at[s, tag + w]).wait()

            lhs = lambda: xb[s, rows, :]

            def putter(buf):
                def put(at, val):
                    buf[rows, at] = val
                return put

            def once(idx):
                @pl.when(jnp.logical_and(s == 0, b == 0))
                def _():
                    w_copies[idx].wait()
            once(0)
            matmul(lhs, wq, putter(q))
            once(1)
            matmul(lhs, wk, putter(k), norm_rope(q, base, 0))
            once(2)
            matmul(lhs, wv, putter(v), norm_rope(k, base, 1))
            return 0
        lax.fori_loop(0, chips, project, 0)

        def finish(b, _):
            hop = hop_of(b, far + [0])
            c = lax.rem(chip + hop, chips)
            base = pl.multiple_of(c * rows_blk, rows_blk)
            rows = pl.ds(base, rows_blk)
            for blk in range(chips):
                @pl.when(c == blk)
                def _():
                    attend(blk)

            def put(at, val):
                a_buf[:, at] = val
            @pl.when(jnp.logical_and(s == 0, b == 0))
            def _():
                w_copies[3].wait()
            matmul(lambda: q[rows, :], wo, put)

            def out_rows(i, _):
                at = pl.ds(pl.multiple_of(i * RC, RC), RC)
                xat = pl.ds(pl.multiple_of(base + i * RC, RC), RC)
                load = lambda h: a_buf[at, h * HEAD_DIM:(h + 1) * HEAD_DIM].astype(jnp.float32)
                rs = sum_sq(load)
                for h in range(heads):
                    cols = slice(h * HEAD_DIM, (h + 1) * HEAD_DIM)
                    res = xb[s, xat, cols].astype(jnp.float32)
                    xb[s, xat, cols] = (res + load(h) * rs * gains_ref[2:3, cols].astype(jnp.float32)).astype(jnp.bfloat16)
                return 0
            lax.fori_loop(0, rows_blk // RC, out_rows, 0)

            def send(w):
                to = c * CORES + (core if w == 0 else 1 - core)
                src = xb.at[s, pl.ds(pl.multiple_of(to * t_loc, t_loc), t_loc)]
                pltpu.make_async_remote_copy(src_ref=src, dst_ref=y_hbm.at[me * n_seq + s], send_sem=y_send.at[s, hop * CORES + w],
                                             recv_sem=y_recv.at[s, hop * CORES + w], device_id={"sp": to}, device_id_type=MESH).start()

            @pl.when(hop == 0)
            def _():
                src = xb.at[s, pl.ds(pl.multiple_of(me * t_loc, t_loc), t_loc)]
                pltpu.make_async_copy(src, y_hbm.at[me * n_seq + s], y_recv.at[s, 0]).start()
                send(1)

            @pl.when(hop != 0)
            def _():
                send(0)
                send(1)
            return 0
        lax.fori_loop(0, chips, finish, 0)
        return 0

    lax.fori_loop(0, n_seq, sequence, 0)

    for s in range(n_seq):
        for tag in range(n):
            pltpu.make_async_copy(xb.at[s, pl.ds(0, t_loc)], y_hbm.at[0], y_recv.at[s, tag]).wait()
    for s in range(n_seq):
        for tag in range(1, n):
            pltpu.make_async_copy(xb.at[s, pl.ds(0, t_loc)], y_hbm.at[0], y_send.at[s, tag]).wait()
    for cp in sends:
        cp.wait_send()


def solution(mesh):
    n = mesh.shape["sp"]

    def local_block(x_loc, pos_loc, w_query, w_key, w_value, w_out, gain_q, gain_k, gain_out):
        batch, t_loc, width = x_loc.shape
        n_seq = batch // n
        inv_freq = 1.0 / (ROPE_THETA ** (np.arange(0, HEAD_DIM, 2, dtype=np.float32) / HEAD_DIM))
        freq = jnp.asarray(np.concatenate([inv_freq, inv_freq]).astype(np.float32)[None, :])
        hbm = pl.BlockSpec(memory_space=pl.ANY)
        vmem = pl.BlockSpec(memory_space=pltpu.VMEM)
        seq = n * t_loc
        bf16 = jnp.bfloat16
        return pl.pallas_call(
            functools.partial(block_kernel, n),
            out_shape=jax.ShapeDtypeStruct(x_loc.shape, bf16),
            in_specs=[hbm, hbm, vmem, vmem, hbm, hbm, hbm, hbm],
            out_specs=hbm,
            scratch_shapes=[
                pltpu.VMEM((width, width), bf16), pltpu.VMEM((width, width), bf16), pltpu.VMEM((width, width), bf16), pltpu.VMEM((width, width), bf16),
                pltpu.VMEM((n_seq, seq, width), bf16),
                pltpu.VMEM((seq, width), bf16), pltpu.VMEM((seq, width), bf16), pltpu.VMEM((seq, width), bf16),
                pltpu.VMEM((CORES * t_loc, width), bf16),
                pltpu.VMEM((2, CORES * t_loc, seq), jnp.float32), pltpu.VMEM((2, CORES * t_loc, seq), bf16),
                pltpu.VMEM((n, batch, t_loc), jnp.int32),
                pltpu.VMEM((seq, HEAD_DIM), jnp.float32), pltpu.VMEM((seq, HEAD_DIM), jnp.float32),
                pltpu.SemaphoreType.DMA((4,)),
                pltpu.SemaphoreType.DMA((n,)), pltpu.SemaphoreType.DMA((n,)),
                pltpu.SemaphoreType.DMA((n_seq, n)), pltpu.SemaphoreType.DMA((n_seq, n)),
                pltpu.SemaphoreType.DMA((n_seq, n)), pltpu.SemaphoreType.DMA((n_seq, n)),
            ],
            compiler_params=pltpu.CompilerParams(collective_id=0, has_side_effects=True, vmem_limit_bytes=VMEM_LIMIT),
            name="attention_block",
        )(x_loc, pos_loc, freq, jnp.stack([gain_q, gain_k, gain_out]), w_query, w_key, w_value, w_out)

    tok_spec = P("dp", "sp", None)
    return jax.shard_map(local_block, mesh=mesh, in_specs=(tok_spec, P("dp", "sp"), P(), P(), P(), P(), P(), P(), P()), out_specs=tok_spec, check_vma=False)
```

```python
import functools
import math

import jax
import jax.numpy as jnp
import numpy as np
from jax import lax
from jax.experimental import pallas as pl
from jax.experimental.pallas import tpu as pltpu
from jax.sharding import PartitionSpec as P

HEAD_DIM = 128
ROPE_THETA = 500000.0
NORM_EPS = 1e-6
SCALE = HEAD_DIM ** -0.5
EXP2_SCALE = SCALE * math.log2(math.e)
CORES = 2
MESH = pl.DeviceIdType.MESH
VMEM_LIMIT = 67043328
NT = 1024
RG = 32
POST_U = 4
YRC = 8

PIO2 = (1.5703125, 4.837512969970703125e-4, 7.54978995489188216e-8)


def cos_sin_rows(angles, lane_low):
    quad = jnp.floor(angles * (2.0 / math.pi) + 0.5)
    r = angles - quad * PIO2[0]
    r = r - quad * PIO2[1]
    r = r - quad * PIO2[2]
    r2 = r * r
    sin_r = r + r * r2 * (-1.6666654611e-1 + r2 * (8.3321608736e-3 + r2 * -1.9515295891e-4))
    cos_r = 1.0 - 0.5 * r2 + r2 * r2 * (4.166664568298827e-2 + r2 * (-1.388731625493765e-3 + r2 * 2.443315711809948e-5))
    quad = jnp.where(lane_low, quad, quad + 3.0)
    quad = quad - 4.0 * jnp.floor(quad * 0.25)
    odd = jnp.logical_or(quad == 1.0, quad == 3.0)
    val = jnp.where(odd, sin_r, cos_r)
    neg = jnp.logical_or(quad == 1.0, quad == 2.0)
    return jnp.where(neg, -val, val)


def block_kernel(n, x_hbm, pos_hbm, freq_ref, gq_ref, gk_ref, ga_ref, wq_hbm, wk_hbm, wv_hbm, wo_hbm, y_hbm,
                 wq, wk, wv, wo, xb, q, k, v, a_buf, s_buf, p_buf, gains_ref, posb, cosb, sinb,
                 w_sem, p_send, p_recv, x_send, x_recv, y_send, y_recv):
    batch, t_loc, width = x_hbm.shape
    n_seq = batch // n
    chips = n // CORES
    rows_blk = CORES * t_loc
    heads = width // HEAD_DIM
    me = lax.axis_index("sp")
    chip = me // CORES
    core = lax.rem(me, CORES)

    def peer(hop, swap):
        other = core if swap == 0 else 1 - core
        return lax.rem(chip + hop, chips) * CORES + other

    peers = [(0, 1)] + [(h, w) for w in range(CORES) for h in (1, chips - 1)] + [(h, w) for h in range(2, chips - 1) for w in range(CORES)]

    w_copies = []
    for idx, (src, dst) in enumerate(((wq_hbm, wq), (wk_hbm, wk), (wv_hbm, wv), (wo_hbm, wo))):
        cp = pltpu.make_async_copy(src, dst, w_sem.at[idx])
        w_copies.append(cp)
    pos_own = pltpu.make_async_copy(pos_hbm, posb.at[me], p_recv.at[0])
    pos_own.start()
    own = [pltpu.make_async_copy(x_hbm.at[me * n_seq + s], xb.at[s, pl.ds(pl.multiple_of(me * t_loc, t_loc), t_loc)], x_recv.at[s, 0]) for s in range(n_seq)]
    for cp in own:
        cp.start()
    for cp in w_copies:
        cp.start()

    sends = []
    barrier = pltpu.get_barrier_semaphore()
    for hop, swap in peers:
        pl.semaphore_signal(barrier, inc=1, device_id={"sp": peer(hop, swap)}, device_id_type=MESH)
    pl.semaphore_wait(barrier, n - 1)
    my_rows = pl.ds(pl.multiple_of(me * t_loc, t_loc), t_loc)
    for hop, swap in peers:
        tag = hop * CORES + swap
        cp = pltpu.make_async_remote_copy(src_ref=pos_hbm, dst_ref=posb.at[me], send_sem=p_send.at[tag], recv_sem=p_recv.at[tag],
                                          device_id={"sp": peer(hop, swap)}, device_id_type=MESH)
        cp.start()
        sends.append(cp)
    for s in range(n_seq):
        for hop, swap in peers:
            tag = hop * CORES + swap
            to = peer(hop, swap)
            cp = pltpu.make_async_remote_copy(src_ref=x_hbm.at[to * n_seq + s], dst_ref=xb.at[s, my_rows],
                                              send_sem=x_send.at[s, tag], recv_sem=x_recv.at[s, tag],
                                              device_id={"sp": to}, device_id_type=MESH)
            cp.start()
            sends.append(cp)

    for idx, g_ref in enumerate((gq_ref, gk_ref, ga_ref)):
        gains_ref[idx:idx + 1, :] = g_ref[...].astype(jnp.float32).reshape(1, width)

    pos_own.wait()
    for tag in range(1, n):
        pltpu.make_async_copy(pos_hbm, posb.at[0], p_recv.at[tag]).wait()

    lane = lax.broadcasted_iota(jnp.int32, (t_loc, HEAD_DIM), 1)
    row = lax.broadcasted_iota(jnp.int32, (t_loc, HEAD_DIM), 0)
    lane_low = lane < HEAD_DIM // 2
    eye = lane == row

    def table_rows(s, j):
        pos_row = posb[j, pl.ds(me * n_seq + s, 1), :].astype(jnp.float32)
        pos_col = jnp.sum(jnp.where(eye, jnp.broadcast_to(pos_row, (t_loc, HEAD_DIM)), 0.0), axis=1, keepdims=True)
        both = cos_sin_rows(pos_col * freq_ref[...], lane_low)
        turned = pltpu.roll(both, HEAD_DIM // 2, 1)
        at = pl.ds(pl.multiple_of(j * t_loc, t_loc), t_loc)
        cosb[at, :] = jnp.where(lane_low, both, turned)
        sinb[at, :] = jnp.where(lane_low, -turned, both)

    RC = 32
    n_iter = width // NT
    side_rows = rows_blk // n_iter

    def matmul(lhs, w, put, side=None):
        def one(j, _):
            at = pl.ds(pl.multiple_of(j * NT, NT), NT)
            put(at, jnp.dot(lhs(), w[:, at], preferred_element_type=jnp.float32).astype(jnp.bfloat16))
            if side is not None:
                side(j)
            return 0
        lax.fori_loop(0, n_iter, one, 0)

    def sum_sq(load):
        total = None
        for h in range(heads):
            t = load(h)
            total = t * t if total is None else total + t * t
        return lax.rsqrt(jnp.sum(total, axis=1, keepdims=True) * (1.0 / width) + NORM_EPS)

    def norm_rope(buf, base, gain):
        def chunk(i):
            at = pl.ds(pl.multiple_of(base + i * RC, RC), RC)
            load = lambda h: buf[at, h * HEAD_DIM:(h + 1) * HEAD_DIM].astype(jnp.float32)
            rs = sum_sq(load)
            cos_t = cosb[at, :]
            sin_t = sinb[at, :]
            for h in range(heads):
                cols = slice(h * HEAD_DIM, (h + 1) * HEAD_DIM)
                t = load(h) * rs * gains_ref[gain:gain + 1, cols]
                buf[at, cols] = (t * cos_t + pltpu.roll(t, HEAD_DIM // 2, 1) * sin_t).astype(jnp.bfloat16)

        def one(j):
            for i in range(side_rows // RC):
                chunk(j * (side_rows // RC) + i)
        return one

    def attend(blk):
        r0 = blk * rows_blk
        kv = r0 + rows_blk
        tri = lax.broadcasted_iota(jnp.int32, (RG, rows_blk), 1) - lax.broadcasted_iota(jnp.int32, (RG, rows_blk), 0)

        def cols_of(h):
            if isinstance(h, int):
                return slice(h * HEAD_DIM, (h + 1) * HEAD_DIM)
            return pl.ds(pl.multiple_of(h * HEAD_DIM, HEAD_DIM), HEAD_DIM)

        def scores(h, slot):
            cols = cols_of(h)
            s_buf[slot, :, 0:kv] = lax.dot_general(q[r0:kv, cols], k[0:kv, cols], (((1,), (1,)), ((), ())), preferred_element_type=jnp.float32)

        def soft(slot):
            for g in range(rows_blk // RG):
                s = s_buf[slot, g * RG:(g + 1) * RG, 0:kv]
                last = jnp.where(tri <= g * RG, s[:, r0:], -1e30)
                s = last if r0 == 0 else jnp.concatenate([s[:, :r0], last], axis=1)
                m = jnp.max(s, axis=1, keepdims=True)
                p = jnp.exp2((s - m) * EXP2_SCALE)
                p_buf[slot, g * RG:(g + 1) * RG, 0:kv] = (p * (1.0 / jnp.sum(p, axis=1, keepdims=True))).astype(jnp.bfloat16)

        def mix(h, slot):
            cols = cols_of(h)
            first = h - slot
            both = slice(first * HEAD_DIM, (first + 2) * HEAD_DIM) if isinstance(h, int) else pl.ds(pl.multiple_of(first * HEAD_DIM, 2 * HEAD_DIM), 2 * HEAD_DIM)
            o = jnp.dot(p_buf[slot, :, 0:kv], v[0:kv, both], preferred_element_type=jnp.float32)
            q[r0:kv, cols] = o[:, slot * HEAD_DIM:(slot + 1) * HEAD_DIM].astype(jnp.bfloat16)

        scores(0, 0)
        scores(1, 1)
        soft(0)

        def pair(i, _):
            for u in range(2):
                h = 2 + 2 * i + u
                scores(h, u)
                soft(1 - u)
                mix(h - 2, u)
            return 0
        lax.fori_loop(0, heads // 2 - 1, pair, 0)
        soft(1)
        mix(heads - 2, 0)
        mix(heads - 1, 1)

    def hop_of(b, order):
        hop = order[-1]
        for i in range(len(order) - 1):
            hop = jnp.where(b == i, order[i], hop)
        return hop

    near = [h for h in (1, chips - 1)] + list(range(2, chips - 1))
    far = near[2:] + near[:2]

    def sequence(s, _):

        def project(b, _):
            hop = hop_of(b, [0] + near)
            c = lax.rem(chip + hop, chips)
            tag = lax.rem(chips - hop, chips) * CORES
            base = pl.multiple_of(c * rows_blk, rows_blk)
            rows = pl.ds(base, rows_blk)

            @pl.when(hop == 0)
            def _():
                pltpu.make_async_copy(x_hbm.at[0], xb.at[s, pl.ds(0, t_loc)], x_recv.at[s, 0]).wait()
                pltpu.make_async_copy(x_hbm.at[0], xb.at[s, pl.ds(0, t_loc)], x_recv.at[s, 1]).wait()

            @pl.when(hop != 0)
            def _():
                for w in range(CORES):
                    pltpu.make_async_copy(x_hbm.at[0], xb.at[s, pl.ds(0, t_loc)], x_recv.at[s, tag + w]).wait()

            lhs = lambda: xb[s, rows, :]

            def putter(buf):
                def put(at, val):
                    buf[rows, at] = val
                return put

            def once(idx):
                @pl.when(jnp.logical_and(s == 0, b == 0))
                def _():
                    w_copies[idx].wait()
            once(0)
            matmul(lhs, wq, putter(q), (lambda j: table_rows(s, c * CORES + j)))
            once(1)
            matmul(lhs, wk, putter(k), norm_rope(q, base, 0))
            once(2)
            matmul(lhs, wv, putter(v), norm_rope(k, base, 1))
            return 0
        lax.fori_loop(0, chips, project, 0)

        def finish(b, _):
            hop = hop_of(b, far + [0])
            c = lax.rem(chip + hop, chips)
            base = pl.multiple_of(c * rows_blk, rows_blk)
            rows = pl.ds(base, rows_blk)
            for blk in range(chips):
                @pl.when(c == blk)
                def _():
                    attend(blk)

            def put(at, val):
                a_buf[:, at] = val
            @pl.when(jnp.logical_and(s == 0, b == 0))
            def _():
                w_copies[3].wait()
            matmul(lambda: q[rows, :], wo, put)

            def out_rows(i):
                at = pl.ds(pl.multiple_of(i * RC, RC), RC)
                xat = pl.ds(pl.multiple_of(base + i * RC, RC), RC)
                load = lambda h: a_buf[at, h * HEAD_DIM:(h + 1) * HEAD_DIM].astype(jnp.float32)
                rs = sum_sq(load)
                for h in range(heads):
                    cols = slice(h * HEAD_DIM, (h + 1) * HEAD_DIM)
                    res = xb[s, xat, cols].astype(jnp.float32)
                    xb[s, xat, cols] = (res + load(h) * rs * gains_ref[2:3, cols]).astype(jnp.bfloat16)

            def out_group(i, _):
                for u in range(POST_U):
                    out_rows(i * POST_U + u)
                return 0
            lax.fori_loop(0, rows_blk // RC // POST_U, out_group, 0)

            def send(w):
                to = c * CORES + (core if w == 0 else 1 - core)
                src = xb.at[s, pl.ds(pl.multiple_of(to * t_loc, t_loc), t_loc)]
                pltpu.make_async_remote_copy(src_ref=src, dst_ref=y_hbm.at[me * n_seq + s], send_sem=y_send.at[s, hop * CORES + w],
                                             recv_sem=y_recv.at[s, hop * CORES + w], device_id={"sp": to}, device_id_type=MESH).start()

            @pl.when(hop == 0)
            def _():
                src = xb.at[s, pl.ds(pl.multiple_of(me * t_loc, t_loc), t_loc)]
                pltpu.make_async_copy(src, y_hbm.at[me * n_seq + s], y_recv.at[s, 0]).start()
                send(1)

            @pl.when(hop != 0)
            def _():
                send(0)
                send(1)
            return 0
        lax.fori_loop(0, chips, finish, 0)
        return 0

    lax.fori_loop(0, n_seq, sequence, 0)

    for s in range(n_seq):
        for tag in range(n):
            pltpu.make_async_copy(xb.at[s, pl.ds(0, t_loc)], y_hbm.at[0], y_recv.at[s, tag]).wait()
    for s in range(n_seq):
        for tag in range(1, n):
            pltpu.make_async_copy(xb.at[s, pl.ds(0, t_loc)], y_hbm.at[0], y_send.at[s, tag]).wait()
    for cp in sends:
        cp.wait_send()


def copy_kernel(parts, src, dst, buf, in_sem, out_sem):
    step = src.shape[0] // parts
    reads = [pltpu.make_async_copy(src.at[pl.ds(i * step, step)], buf.at[pl.ds(i * step, step)], in_sem.at[i]) for i in range(parts)]
    writes = [pltpu.make_async_copy(buf.at[pl.ds(i * step, step)], dst.at[pl.ds(i * step, step)], out_sem.at[i]) for i in range(parts)]
    for cp in reads:
        cp.start()
    for i in range(parts):
        reads[i].wait()
        writes[i].start()
    for cp in writes:
        cp.wait()


def solution(mesh):
    n = mesh.shape["sp"]

    def local_block(x_loc, pos_loc, w_query, w_key, w_value, w_out, gain_q, gain_k, gain_out):
        batch, t_loc, width = x_loc.shape
        n_seq = batch // n
        inv_freq = 1.0 / (ROPE_THETA ** (np.arange(0, HEAD_DIM, 2, dtype=np.float32) / HEAD_DIM))
        freq = jnp.asarray(np.concatenate([inv_freq, inv_freq]).astype(np.float32)[None, :])
        hbm = pl.BlockSpec(memory_space=pl.ANY)
        vmem = pl.BlockSpec(memory_space=pltpu.VMEM)
        seq = n * t_loc
        bf16 = jnp.bfloat16
        y_loc = pl.pallas_call(
            functools.partial(block_kernel, n),
            out_shape=jax.ShapeDtypeStruct(x_loc.shape, bf16),
            in_specs=[hbm, hbm, vmem, vmem, vmem, vmem, hbm, hbm, hbm, hbm],
            out_specs=hbm,
            scratch_shapes=[
                pltpu.VMEM((width, width), bf16), pltpu.VMEM((width, width), bf16), pltpu.VMEM((width, width), bf16), pltpu.VMEM((width, width), bf16),
                pltpu.VMEM((n_seq, seq, width), bf16),
                pltpu.VMEM((seq, width), bf16), pltpu.VMEM((seq, width), bf16), pltpu.VMEM((seq, width), bf16),
                pltpu.VMEM((CORES * t_loc, width), bf16),
                pltpu.VMEM((2, CORES * t_loc, seq), jnp.float32), pltpu.VMEM((2, CORES * t_loc, seq), bf16),
                pltpu.VMEM((3, width), jnp.float32),
                pltpu.VMEM((n, batch, t_loc), jnp.int32),
                pltpu.VMEM((seq, HEAD_DIM), jnp.float32), pltpu.VMEM((seq, HEAD_DIM), jnp.float32),
                pltpu.SemaphoreType.DMA((4,)),
                pltpu.SemaphoreType.DMA((n,)), pltpu.SemaphoreType.DMA((n,)),
                pltpu.SemaphoreType.DMA((n_seq, n)), pltpu.SemaphoreType.DMA((n_seq, n)),
                pltpu.SemaphoreType.DMA((n_seq, n)), pltpu.SemaphoreType.DMA((n_seq, n)),
            ],
            compiler_params=pltpu.CompilerParams(collective_id=0, has_side_effects=True, vmem_limit_bytes=VMEM_LIMIT),
            name="attention_block",
        )(x_loc, pos_loc, freq, gain_q, gain_k, gain_out, w_query, w_key, w_value, w_out)
        parts = YRC
        return pl.pallas_call(
            functools.partial(copy_kernel, parts),
            out_shape=jax.ShapeDtypeStruct(x_loc.shape, bf16),
            in_specs=[hbm],
            out_specs=hbm,
            scratch_shapes=[pltpu.VMEM(x_loc.shape, bf16), pltpu.SemaphoreType.DMA((parts,)), pltpu.SemaphoreType.DMA((parts,))],
            compiler_params=pltpu.CompilerParams(vmem_limit_bytes=VMEM_LIMIT),
            name="result_copy",
        )(y_loc)

    tok_spec = P("dp", "sp", None)
    return jax.shard_map(local_block, mesh=mesh, in_specs=(tok_spec, P("dp", "sp"), P(), P(), P(), P(), P(), P(), P()), out_specs=tok_spec, check_vma=False)
```

```python
import functools
import math

import jax
import jax.numpy as jnp
import numpy as np
from jax import lax
from jax.experimental import pallas as pl
from jax.experimental.pallas import tpu as pltpu
from jax.sharding import PartitionSpec as P

HEAD_DIM = 128
ROPE_THETA = 500000.0
NORM_EPS = 1e-6
SCALE = HEAD_DIM ** -0.5
EXP2_SCALE = SCALE * math.log2(math.e)
CORES = 2
MESH = pl.DeviceIdType.MESH
VMEM_LIMIT = 67043328
NT = 1024
RG = 32
POST_U = 4

PIO2 = (1.5703125, 4.837512969970703125e-4, 7.54978995489188216e-8)


def cos_sin_rows(angles, lane_low):
    quad = jnp.floor(angles * (2.0 / math.pi) + 0.5)
    r = angles - quad * PIO2[0]
    r = r - quad * PIO2[1]
    r = r - quad * PIO2[2]
    r2 = r * r
    sin_r = r + r * r2 * (-1.6666654611e-1 + r2 * (8.3321608736e-3 + r2 * -1.9515295891e-4))
    cos_r = 1.0 - 0.5 * r2 + r2 * r2 * (4.166664568298827e-2 + r2 * (-1.388731625493765e-3 + r2 * 2.443315711809948e-5))
    quad = jnp.where(lane_low, quad, quad + 3.0)
    quad = quad - 4.0 * jnp.floor(quad * 0.25)
    odd = jnp.logical_or(quad == 1.0, quad == 3.0)
    val = jnp.where(odd, sin_r, cos_r)
    neg = jnp.logical_or(quad == 1.0, quad == 2.0)
    return jnp.where(neg, -val, val)


def block_kernel(n, x_hbm, pos_hbm, freq_hbm, gq_hbm, gk_hbm, ga_hbm, wq_hbm, wk_hbm, wv_hbm, wo_hbm, y_early, y_last,
                 wq, wk, wv, wo, xb, q, k, v, a_buf, s_buf, p_buf, freq_ref, gq_ref, gk_ref, ga_ref, gains_ref, posb, cosb, sinb,
                 w_sem, g_sem, p_send, p_recv, x_send, x_recv, y_send, y_recv):
    batch, t_loc, width = x_hbm.shape
    n_seq = batch // n
    chips = n // CORES
    rows_blk = CORES * t_loc
    heads = width // HEAD_DIM
    y_outs = [y_early.at[s] for s in range(n_seq - 1)] + [y_last]
    me = lax.axis_index("sp")
    chip = me // CORES
    core = lax.rem(me, CORES)

    def peer(hop, swap):
        other = core if swap == 0 else 1 - core
        return lax.rem(chip + hop, chips) * CORES + other

    peers = [(0, 1)] + [(h, w) for w in range(CORES) for h in (1, chips - 1)] + [(h, w) for h in range(2, chips - 1) for w in range(CORES)]

    barrier = pltpu.get_barrier_semaphore()
    for hop, swap in peers:
        pl.semaphore_signal(barrier, inc=1, device_id={"sp": peer(hop, swap)}, device_id_type=MESH)

    w_copies = []
    for idx, (src, dst) in enumerate(((wq_hbm, wq), (wk_hbm, wk), (wv_hbm, wv), (wo_hbm, wo))):
        cp = pltpu.make_async_copy(src, dst, w_sem.at[idx])
        w_copies.append(cp)
    pos_own = pltpu.make_async_copy(pos_hbm, posb.at[me], p_recv.at[0])
    pos_own.start()
    own = [pltpu.make_async_copy(x_hbm.at[me * n_seq + s], xb.at[s, pl.ds(pl.multiple_of(me * t_loc, t_loc), t_loc)], x_recv.at[s, 0]) for s in range(n_seq)]
    for cp in own:
        cp.start()
    small = []
    for idx, (src, dst) in enumerate(((freq_hbm, freq_ref), (gq_hbm, gq_ref), (gk_hbm, gk_ref), (ga_hbm, ga_ref))):
        cp = pltpu.make_async_copy(src, dst, g_sem.at[idx])
        cp.start()
        small.append(cp)
    for cp in w_copies:
        cp.start()

    sends = []
    pl.semaphore_wait(barrier, n - 1)
    my_rows = pl.ds(pl.multiple_of(me * t_loc, t_loc), t_loc)
    for hop, swap in peers:
        tag = hop * CORES + swap
        cp = pltpu.make_async_remote_copy(src_ref=pos_hbm, dst_ref=posb.at[me], send_sem=p_send.at[tag], recv_sem=p_recv.at[tag],
                                          device_id={"sp": peer(hop, swap)}, device_id_type=MESH)
        cp.start()
        sends.append(cp)
    for s in range(n_seq):
        for hop, swap in peers:
            tag = hop * CORES + swap
            to = peer(hop, swap)
            cp = pltpu.make_async_remote_copy(src_ref=x_hbm.at[to * n_seq + s], dst_ref=xb.at[s, my_rows],
                                              send_sem=x_send.at[s, tag], recv_sem=x_recv.at[s, tag],
                                              device_id={"sp": to}, device_id_type=MESH)
            cp.start()
            sends.append(cp)

    for cp in small:
        cp.wait()
    for idx, g_ref in enumerate((gq_ref, gk_ref, ga_ref)):
        gains_ref[idx:idx + 1, :] = g_ref[...].astype(jnp.float32).reshape(1, width)

    pos_own.wait()
    for tag in range(1, n):
        pltpu.make_async_copy(pos_hbm, posb.at[0], p_recv.at[tag]).wait()

    lane = lax.broadcasted_iota(jnp.int32, (t_loc, HEAD_DIM), 1)
    row = lax.broadcasted_iota(jnp.int32, (t_loc, HEAD_DIM), 0)
    lane_low = lane < HEAD_DIM // 2
    eye = lane == row

    def table_rows(s, j):
        pos_row = posb[j, pl.ds(me * n_seq + s, 1), :].astype(jnp.float32)
        pos_col = jnp.sum(jnp.where(eye, jnp.broadcast_to(pos_row, (t_loc, HEAD_DIM)), 0.0), axis=1, keepdims=True)
        both = cos_sin_rows(pos_col * freq_ref[...], lane_low)
        turned = pltpu.roll(both, HEAD_DIM // 2, 1)
        at = pl.ds(pl.multiple_of(j * t_loc, t_loc), t_loc)
        cosb[at, :] = jnp.where(lane_low, both, turned)
        sinb[at, :] = jnp.where(lane_low, -turned, both)

    RC = 32
    n_iter = width // NT
    side_rows = rows_blk // n_iter

    def matmul(lhs, w, put, side=None):
        def one(j, _):
            at = pl.ds(pl.multiple_of(j * NT, NT), NT)
            put(at, jnp.dot(lhs(), w[:, at], preferred_element_type=jnp.float32).astype(jnp.bfloat16))
            if side is not None:
                side(j)
            return 0
        lax.fori_loop(0, n_iter, one, 0)

    def sum_sq(load):
        total = None
        for h in range(heads):
            t = load(h)
            total = t * t if total is None else total + t * t
        return lax.rsqrt(jnp.sum(total, axis=1, keepdims=True) * (1.0 / width) + NORM_EPS)

    def norm_rope(buf, base, gain):
        def chunk(i):
            at = pl.ds(pl.multiple_of(base + i * RC, RC), RC)
            load = lambda h: buf[at, h * HEAD_DIM:(h + 1) * HEAD_DIM].astype(jnp.float32)
            rs = sum_sq(load)
            cos_t = cosb[at, :]
            sin_t = sinb[at, :]
            for h in range(heads):
                cols = slice(h * HEAD_DIM, (h + 1) * HEAD_DIM)
                t = load(h) * rs * gains_ref[gain:gain + 1, cols]
                buf[at, cols] = (t * cos_t + pltpu.roll(t, HEAD_DIM // 2, 1) * sin_t).astype(jnp.bfloat16)

        def one(j):
            for i in range(side_rows // RC):
                chunk(j * (side_rows // RC) + i)
        return one

    def attend(blk):
        r0 = blk * rows_blk
        kv = r0 + rows_blk
        tri = lax.broadcasted_iota(jnp.int32, (RG, rows_blk), 1) - lax.broadcasted_iota(jnp.int32, (RG, rows_blk), 0)

        def cols_of(h):
            if isinstance(h, int):
                return slice(h * HEAD_DIM, (h + 1) * HEAD_DIM)
            return pl.ds(pl.multiple_of(h * HEAD_DIM, HEAD_DIM), HEAD_DIM)

        def scores(h, slot):
            cols = cols_of(h)
            s_buf[slot, :, 0:kv] = lax.dot_general(q[r0:kv, cols], k[0:kv, cols], (((1,), (1,)), ((), ())), preferred_element_type=jnp.float32)

        def soft(slot):
            for g in range(rows_blk // RG):
                s = s_buf[slot, g * RG:(g + 1) * RG, 0:kv]
                last = jnp.where(tri <= g * RG, s[:, r0:], -1e30)
                s = last if r0 == 0 else jnp.concatenate([s[:, :r0], last], axis=1)
                m = jnp.max(s, axis=1, keepdims=True)
                p = jnp.exp2((s - m) * EXP2_SCALE)
                p_buf[slot, g * RG:(g + 1) * RG, 0:kv] = (p * (1.0 / jnp.sum(p, axis=1, keepdims=True))).astype(jnp.bfloat16)

        def mix(h, slot):
            cols = cols_of(h)
            first = h - slot
            both = slice(first * HEAD_DIM, (first + 2) * HEAD_DIM) if isinstance(h, int) else pl.ds(pl.multiple_of(first * HEAD_DIM, 2 * HEAD_DIM), 2 * HEAD_DIM)
            o = jnp.dot(p_buf[slot, :, 0:kv], v[0:kv, both], preferred_element_type=jnp.float32)
            q[r0:kv, cols] = o[:, slot * HEAD_DIM:(slot + 1) * HEAD_DIM].astype(jnp.bfloat16)

        scores(0, 0)
        scores(1, 1)
        soft(0)

        def pair(i, _):
            for u in range(2):
                h = 2 + 2 * i + u
                scores(h, u)
                soft(1 - u)
                mix(h - 2, u)
            return 0
        lax.fori_loop(0, heads // 2 - 1, pair, 0)
        soft(1)
        mix(heads - 2, 0)
        mix(heads - 1, 1)

    def hop_of(b, order):
        hop = order[-1]
        for i in range(len(order) - 1):
            hop = jnp.where(b == i, order[i], hop)
        return hop

    near = [h for h in (1, chips - 1)] + list(range(2, chips - 1))
    far = near[2:] + near[:2]

    def sequence(s, _):

        def project(b, _):
            hop = hop_of(b, [0] + near)
            c = lax.rem(chip + hop, chips)
            tag = lax.rem(chips - hop, chips) * CORES
            base = pl.multiple_of(c * rows_blk, rows_blk)
            rows = pl.ds(base, rows_blk)

            @pl.when(hop == 0)
            def _():
                pltpu.make_async_copy(x_hbm.at[0], xb.at[s, pl.ds(0, t_loc)], x_recv.at[s, 0]).wait()
                pltpu.make_async_copy(x_hbm.at[0], xb.at[s, pl.ds(0, t_loc)], x_recv.at[s, 1]).wait()

            @pl.when(hop != 0)
            def _():
                for w in range(CORES):
                    pltpu.make_async_copy(x_hbm.at[0], xb.at[s, pl.ds(0, t_loc)], x_recv.at[s, tag + w]).wait()

            lhs = lambda: xb[s, rows, :]

            def putter(buf):
                def put(at, val):
                    buf[rows, at] = val
                return put

            def once(idx):
                @pl.when(jnp.logical_and(s == 0, b == 0))
                def _():
                    w_copies[idx].wait()
            once(0)
            matmul(lhs, wq, putter(q), (lambda j: table_rows(s, c * CORES + j)))
            once(1)
            matmul(lhs, wk, putter(k), norm_rope(q, base, 0))
            once(2)
            matmul(lhs, wv, putter(v), norm_rope(k, base, 1))
            return 0
        lax.fori_loop(0, chips, project, 0)

        def finish(b, _):
            hop = hop_of(b, far + [0])
            c = lax.rem(chip + hop, chips)
            base = pl.multiple_of(c * rows_blk, rows_blk)
            rows = pl.ds(base, rows_blk)
            for blk in range(chips):
                @pl.when(c == blk)
                def _():
                    attend(blk)

            def put(at, val):
                a_buf[:, at] = val
            @pl.when(jnp.logical_and(s == 0, b == 0))
            def _():
                w_copies[3].wait()
            matmul(lambda: q[rows, :], wo, put)

            def out_rows(i):
                at = pl.ds(pl.multiple_of(i * RC, RC), RC)
                xat = pl.ds(pl.multiple_of(base + i * RC, RC), RC)
                load = lambda h: a_buf[at, h * HEAD_DIM:(h + 1) * HEAD_DIM].astype(jnp.float32)
                rs = sum_sq(load)
                for h in range(heads):
                    cols = slice(h * HEAD_DIM, (h + 1) * HEAD_DIM)
                    res = xb[s, xat, cols].astype(jnp.float32)
                    xb[s, xat, cols] = (res + load(h) * rs * gains_ref[2:3, cols]).astype(jnp.bfloat16)

            def out_group(i, _):
                for u in range(POST_U):
                    out_rows(i * POST_U + u)
                return 0
            lax.fori_loop(0, rows_blk // RC // POST_U, out_group, 0)

            def send(w, dst):
                to = c * CORES + (core if w == 0 else 1 - core)
                src = xb.at[s, pl.ds(pl.multiple_of(to * t_loc, t_loc), t_loc)]
                pltpu.make_async_remote_copy(src_ref=src, dst_ref=dst.at[me], send_sem=y_send.at[s, hop * CORES + w],
                                             recv_sem=y_recv.at[s, hop * CORES + w], device_id={"sp": to}, device_id_type=MESH).start()

            for s_now in range(n_seq):
                @pl.when(jnp.logical_and(s == s_now, hop == 0))
                def _():
                    src = xb.at[s_now, pl.ds(pl.multiple_of(me * t_loc, t_loc), t_loc)]
                    pltpu.make_async_copy(src, y_outs[s_now].at[me], y_recv.at[s_now, 0]).start()
                    send(1, y_outs[s_now])

                @pl.when(jnp.logical_and(s == s_now, hop != 0))
                def _():
                    send(0, y_outs[s_now])
                    send(1, y_outs[s_now])
            return 0
        lax.fori_loop(0, chips, finish, 0)
        return 0

    lax.fori_loop(0, n_seq, sequence, 0)

    for s in range(n_seq):
        for tag in range(n):
            pltpu.make_async_copy(xb.at[s, pl.ds(0, t_loc)], y_outs[s].at[0], y_recv.at[s, tag]).wait()
    for s in range(n_seq):
        for tag in range(1, n):
            pltpu.make_async_copy(xb.at[s, pl.ds(0, t_loc)], y_outs[s].at[0], y_send.at[s, tag]).wait()
    for cp in sends:
        cp.wait_send()


def copy_kernel(early, last, dst, out_sem):
    others, n = early.shape[:2]
    writes = []
    for i in range(n):
        writes.append(pltpu.make_async_copy(last.at[i], dst.at[i * (others + 1) + others], out_sem.at[others, i]))
        for s in range(others):
            writes.append(pltpu.make_async_copy(early.at[s, i], dst.at[i * (others + 1) + s], out_sem.at[s, i]))
    for cp in writes:
        cp.start()
    for cp in writes:
        cp.wait()


def solution(mesh):
    n = mesh.shape["sp"]

    def local_block(x_loc, pos_loc, w_query, w_key, w_value, w_out, gain_q, gain_k, gain_out):
        batch, t_loc, width = x_loc.shape
        n_seq = batch // n
        inv_freq = 1.0 / (ROPE_THETA ** (np.arange(0, HEAD_DIM, 2, dtype=np.float32) / HEAD_DIM))
        freq = jnp.asarray(np.concatenate([inv_freq, inv_freq]).astype(np.float32)[None, :])
        hbm = pl.BlockSpec(memory_space=pl.ANY)
        seq = n * t_loc
        bf16 = jnp.bfloat16
        early, last = pl.pallas_call(
            functools.partial(block_kernel, n),
            out_shape=(pltpu.HBM((n_seq - 1, n, t_loc, width), bf16), pltpu.VMEM((n, t_loc, width), bf16)),
            in_specs=[hbm] * 10,
            out_specs=(hbm, hbm),
            scratch_shapes=[
                pltpu.VMEM((width, width), bf16), pltpu.VMEM((width, width), bf16), pltpu.VMEM((width, width), bf16), pltpu.VMEM((width, width), bf16),
                pltpu.VMEM((n_seq, seq, width), bf16),
                pltpu.VMEM((seq, width), bf16), pltpu.VMEM((seq, width), bf16), pltpu.VMEM((seq, width), bf16),
                pltpu.VMEM((CORES * t_loc, width), bf16),
                pltpu.VMEM((2, CORES * t_loc, seq), jnp.float32), pltpu.VMEM((2, CORES * t_loc, seq), bf16),
                pltpu.VMEM((1, HEAD_DIM), jnp.float32), pltpu.VMEM((width,), bf16), pltpu.VMEM((width,), bf16), pltpu.VMEM((width,), bf16),
                pltpu.VMEM((3, width), jnp.float32),
                pltpu.VMEM((n, batch, t_loc), jnp.int32),
                pltpu.VMEM((seq, HEAD_DIM), jnp.float32), pltpu.VMEM((seq, HEAD_DIM), jnp.float32),
                pltpu.SemaphoreType.DMA((4,)), pltpu.SemaphoreType.DMA((4,)),
                pltpu.SemaphoreType.DMA((n,)), pltpu.SemaphoreType.DMA((n,)),
                pltpu.SemaphoreType.DMA((n_seq, n)), pltpu.SemaphoreType.DMA((n_seq, n)),
                pltpu.SemaphoreType.DMA((n_seq, n)), pltpu.SemaphoreType.DMA((n_seq, n)),
            ],
            compiler_params=pltpu.CompilerParams(collective_id=0, has_side_effects=True, vmem_limit_bytes=VMEM_LIMIT - seq * width * 2),
            name="attention_block",
        )(x_loc, pos_loc, freq, gain_q, gain_k, gain_out, w_query, w_key, w_value, w_out)
        return pl.pallas_call(
            copy_kernel,
            out_shape=jax.ShapeDtypeStruct(x_loc.shape, bf16),
            in_specs=[pl.BlockSpec(memory_space=pltpu.VMEM), hbm],
            out_specs=hbm,
            scratch_shapes=[pltpu.SemaphoreType.DMA((n_seq, n))],
            compiler_params=pltpu.CompilerParams(vmem_limit_bytes=VMEM_LIMIT // 4),
            name="result_copy",
        )(early, last)

    tok_spec = P("dp", "sp", None)
    return jax.shard_map(local_block, mesh=mesh, in_specs=(tok_spec, P("dp", "sp"), P(), P(), P(), P(), P(), P(), P()), out_specs=tok_spec, check_vma=False)
```

```python
import functools
import math

import jax
import jax.numpy as jnp
import numpy as np
from jax import lax
from jax.experimental import pallas as pl
from jax.experimental.pallas import tpu as pltpu
from jax.sharding import PartitionSpec as P

HEAD_DIM = 128
ROPE_THETA = 500000.0
NORM_EPS = 1e-6
SCALE = HEAD_DIM ** -0.5
EXP2_SCALE = SCALE * math.log2(math.e)
CORES = 2
MESH = pl.DeviceIdType.MESH
VMEM_LIMIT = 67043328
NT = 1024
RG = 32
POST_U = 8

PIO2 = (1.5703125, 4.837512969970703125e-4, 7.54978995489188216e-8)


def cos_sin_rows(angles, lane_low):
    quad = jnp.floor(angles * (2.0 / math.pi) + 0.5)
    r = angles - quad * PIO2[0]
    r = r - quad * PIO2[1]
    r = r - quad * PIO2[2]
    r2 = r * r
    sin_r = r + r * r2 * (-1.6666654611e-1 + r2 * (8.3321608736e-3 + r2 * -1.9515295891e-4))
    cos_r = 1.0 - 0.5 * r2 + r2 * r2 * (4.166664568298827e-2 + r2 * (-1.388731625493765e-3 + r2 * 2.443315711809948e-5))
    quad = jnp.where(lane_low, quad, quad + 3.0)
    quad = quad - 4.0 * jnp.floor(quad * 0.25)
    odd = jnp.logical_or(quad == 1.0, quad == 3.0)
    val = jnp.where(odd, sin_r, cos_r)
    neg = jnp.logical_or(quad == 1.0, quad == 2.0)
    return jnp.where(neg, -val, val)


def block_kernel(n, x_hbm, pos_hbm, freq_hbm, gq_hbm, gk_hbm, ga_hbm, wq_hbm, wk_hbm, wv_hbm, wo_hbm, y_early, y_last,
                 wq, wk, wv, wo, xb, q, k, v, a_buf, s_buf, p_buf, freq_ref, gq_ref, gk_ref, ga_ref, gains_ref, posb, cosb, sinb,
                 w_sem, g_sem, p_send, p_recv, x_send, x_recv, y_send, y_recv):
    batch, t_loc, width = x_hbm.shape
    n_seq = batch // n
    chips = n // CORES
    rows_blk = CORES * t_loc
    heads = width // HEAD_DIM
    y_outs = [y_early.at[s] for s in range(n_seq - 1)] + [y_last]
    me = lax.axis_index("sp")
    chip = me // CORES
    core = lax.rem(me, CORES)

    def peer(hop, swap):
        other = core if swap == 0 else 1 - core
        return lax.rem(chip + hop, chips) * CORES + other

    peers = [(0, 1)] + [(h, w) for w in range(CORES) for h in (1, chips - 1)] + [(h, w) for h in range(2, chips - 1) for w in range(CORES)]

    barrier = pltpu.get_barrier_semaphore()
    for hop, swap in peers:
        pl.semaphore_signal(barrier, inc=1, device_id={"sp": peer(hop, swap)}, device_id_type=MESH)

    w_copies = []
    for idx, (src, dst) in enumerate(((wq_hbm, wq), (wk_hbm, wk), (wv_hbm, wv), (wo_hbm, wo))):
        cp = pltpu.make_async_copy(src, dst, w_sem.at[idx])
        w_copies.append(cp)
    pos_own = pltpu.make_async_copy(pos_hbm, posb.at[me], p_recv.at[0])
    pos_own.start()
    own = [pltpu.make_async_copy(x_hbm.at[me * n_seq + s], xb.at[s, pl.ds(pl.multiple_of(me * t_loc, t_loc), t_loc)], x_recv.at[s, 0]) for s in range(n_seq)]
    for cp in own:
        cp.start()
    small = []
    for idx, (src, dst) in enumerate(((freq_hbm, freq_ref), (gq_hbm, gq_ref), (gk_hbm, gk_ref), (ga_hbm, ga_ref))):
        cp = pltpu.make_async_copy(src, dst, g_sem.at[idx])
        cp.start()
        small.append(cp)
    for cp in w_copies:
        cp.start()

    sends = []
    pl.semaphore_wait(barrier, n - 1)
    my_rows = pl.ds(pl.multiple_of(me * t_loc, t_loc), t_loc)
    for hop, swap in peers:
        tag = hop * CORES + swap
        cp = pltpu.make_async_remote_copy(src_ref=pos_hbm, dst_ref=posb.at[me], send_sem=p_send.at[tag], recv_sem=p_recv.at[tag],
                                          device_id={"sp": peer(hop, swap)}, device_id_type=MESH)
        cp.start()
        sends.append(cp)
    for s in range(n_seq):
        for hop, swap in peers:
            tag = hop * CORES + swap
            to = peer(hop, swap)
            cp = pltpu.make_async_remote_copy(src_ref=x_hbm.at[to * n_seq + s], dst_ref=xb.at[s, my_rows],
                                              send_sem=x_send.at[s, tag], recv_sem=x_recv.at[s, tag],
                                              device_id={"sp": to}, device_id_type=MESH)
            cp.start()
            sends.append(cp)

    for cp in small:
        cp.wait()
    for idx, g_ref in enumerate((gq_ref, gk_ref, ga_ref)):
        gains_ref[idx:idx + 1, :] = g_ref[...].astype(jnp.float32).reshape(1, width)

    pos_own.wait()
    for tag in range(1, n):
        pltpu.make_async_copy(pos_hbm, posb.at[0], p_recv.at[tag]).wait()

    lane = lax.broadcasted_iota(jnp.int32, (t_loc, HEAD_DIM), 1)
    row = lax.broadcasted_iota(jnp.int32, (t_loc, HEAD_DIM), 0)
    lane_low = lane < HEAD_DIM // 2
    eye = lane == row

    def table_rows(s, j):
        pos_row = posb[j, pl.ds(me * n_seq + s, 1), :].astype(jnp.float32)
        pos_col = jnp.sum(jnp.where(eye, jnp.broadcast_to(pos_row, (t_loc, HEAD_DIM)), 0.0), axis=1, keepdims=True)
        both = cos_sin_rows(pos_col * freq_ref[...], lane_low)
        turned = pltpu.roll(both, HEAD_DIM // 2, 1)
        at = pl.ds(pl.multiple_of(j * t_loc, t_loc), t_loc)
        cosb[at, :] = jnp.where(lane_low, both, turned)
        sinb[at, :] = jnp.where(lane_low, -turned, both)

    RC = 32
    n_iter = width // NT
    side_rows = rows_blk // n_iter

    def matmul(lhs, w, put, side=None):
        def one(j, _):
            at = pl.ds(pl.multiple_of(j * NT, NT), NT)
            put(at, jnp.dot(lhs(), w[:, at], preferred_element_type=jnp.float32).astype(jnp.bfloat16))
            if side is not None:
                side(j)
            return 0
        lax.fori_loop(0, n_iter, one, 0)

    def sum_sq(load):
        total = None
        for h in range(heads):
            t = load(h)
            total = t * t if total is None else total + t * t
        return lax.rsqrt(jnp.sum(total, axis=1, keepdims=True) * (1.0 / width) + NORM_EPS)

    def norm_rope(buf, base, gain):
        def chunk(i):
            at = pl.ds(pl.multiple_of(base + i * RC, RC), RC)
            load = lambda h: buf[at, h * HEAD_DIM:(h + 1) * HEAD_DIM].astype(jnp.float32)
            rs = sum_sq(load)
            cos_t = cosb[at, :]
            sin_t = sinb[at, :]
            for h in range(heads):
                cols = slice(h * HEAD_DIM, (h + 1) * HEAD_DIM)
                t = load(h) * rs * gains_ref[gain:gain + 1, cols]
                buf[at, cols] = (t * cos_t + pltpu.roll(t, HEAD_DIM // 2, 1) * sin_t).astype(jnp.bfloat16)

        def one(j):
            for i in range(side_rows // RC):
                chunk(j * (side_rows // RC) + i)
        return one

    def attend(blk):
        r0 = blk * rows_blk
        kv = r0 + rows_blk
        tri = lax.broadcasted_iota(jnp.int32, (RG, rows_blk), 1) - lax.broadcasted_iota(jnp.int32, (RG, rows_blk), 0)

        def cols_of(h):
            if isinstance(h, int):
                return slice(h * HEAD_DIM, (h + 1) * HEAD_DIM)
            return pl.ds(pl.multiple_of(h * HEAD_DIM, HEAD_DIM), HEAD_DIM)

        def scores(h, slot):
            cols = cols_of(h)
            s_buf[slot, :, 0:kv] = lax.dot_general(q[r0:kv, cols], k[0:kv, cols], (((1,), (1,)), ((), ())), preferred_element_type=jnp.float32)

        def soft(slot):
            for g in range(rows_blk // RG):
                s = s_buf[slot, g * RG:(g + 1) * RG, 0:kv]
                last = jnp.where(tri <= g * RG, s[:, r0:], -1e30)
                s = last if r0 == 0 else jnp.concatenate([s[:, :r0], last], axis=1)
                m = jnp.max(s, axis=1, keepdims=True)
                p = jnp.exp2((s - m) * EXP2_SCALE)
                p_buf[slot, g * RG:(g + 1) * RG, 0:kv] = (p * (1.0 / jnp.sum(p, axis=1, keepdims=True))).astype(jnp.bfloat16)

        def mix(h, slot):
            cols = cols_of(h)
            first = h - slot
            both = slice(first * HEAD_DIM, (first + 2) * HEAD_DIM) if isinstance(h, int) else pl.ds(pl.multiple_of(first * HEAD_DIM, 2 * HEAD_DIM), 2 * HEAD_DIM)
            o = jnp.dot(p_buf[slot, :, 0:kv], v[0:kv, both], preferred_element_type=jnp.float32)
            q[r0:kv, cols] = o[:, slot * HEAD_DIM:(slot + 1) * HEAD_DIM].astype(jnp.bfloat16)

        scores(0, 0)
        scores(1, 1)
        soft(0)

        def pair(i, _):
            for u in range(2):
                h = 2 + 2 * i + u
                scores(h, u)
                soft(1 - u)
                mix(h - 2, u)
            return 0
        lax.fori_loop(0, heads // 2 - 1, pair, 0)
        soft(1)
        mix(heads - 2, 0)
        mix(heads - 1, 1)

    def hop_of(b, order):
        hop = order[-1]
        for i in range(len(order) - 1):
            hop = jnp.where(b == i, order[i], hop)
        return hop

    near = [h for h in (1, chips - 1)] + list(range(2, chips - 1))
    far = near[2:] + near[:2]

    def sequence(s, _):

        def project(b, _):
            hop = hop_of(b, [0] + near)
            c = lax.rem(chip + hop, chips)
            tag = lax.rem(chips - hop, chips) * CORES
            base = pl.multiple_of(c * rows_blk, rows_blk)
            rows = pl.ds(base, rows_blk)

            @pl.when(hop == 0)
            def _():
                pltpu.make_async_copy(x_hbm.at[0], xb.at[s, pl.ds(0, t_loc)], x_recv.at[s, 0]).wait()
                pltpu.make_async_copy(x_hbm.at[0], xb.at[s, pl.ds(0, t_loc)], x_recv.at[s, 1]).wait()

            @pl.when(hop != 0)
            def _():
                for w in range(CORES):
                    pltpu.make_async_copy(x_hbm.at[0], xb.at[s, pl.ds(0, t_loc)], x_recv.at[s, tag + w]).wait()

            lhs = lambda: xb[s, rows, :]

            def putter(buf):
                def put(at, val):
                    buf[rows, at] = val
                return put

            def once(idx):
                @pl.when(jnp.logical_and(s == 0, b == 0))
                def _():
                    w_copies[idx].wait()
            once(0)
            matmul(lhs, wq, putter(q), (lambda j: table_rows(s, c * CORES + j)))
            once(1)
            matmul(lhs, wk, putter(k), norm_rope(q, base, 0))
            once(2)
            matmul(lhs, wv, putter(v), norm_rope(k, base, 1))
            return 0
        lax.fori_loop(0, chips, project, 0)

        def finish(b, _):
            hop = hop_of(b, far + [0])
            c = lax.rem(chip + hop, chips)
            base = pl.multiple_of(c * rows_blk, rows_blk)
            rows = pl.ds(base, rows_blk)
            for blk in range(chips):
                @pl.when(c == blk)
                def _():
                    attend(blk)

            def put(at, val):
                a_buf[:, at] = val
            @pl.when(jnp.logical_and(s == 0, b == 0))
            def _():
                w_copies[3].wait()
            matmul(lambda: q[rows, :], wo, put)

            def out_rows(i):
                at = pl.ds(pl.multiple_of(i * RC, RC), RC)
                xat = pl.ds(pl.multiple_of(base + i * RC, RC), RC)
                load = lambda h: a_buf[at, h * HEAD_DIM:(h + 1) * HEAD_DIM].astype(jnp.float32)
                rs = sum_sq(load)
                for h in range(heads):
                    cols = slice(h * HEAD_DIM, (h + 1) * HEAD_DIM)
                    res = xb[s, xat, cols].astype(jnp.float32)
                    xb[s, xat, cols] = (res + load(h) * rs * gains_ref[2:3, cols]).astype(jnp.bfloat16)

            def out_group(i, _):
                for u in range(POST_U):
                    out_rows(i * POST_U + u)
                return 0
            lax.fori_loop(0, rows_blk // RC // POST_U, out_group, 0)

            def send(w, dst):
                to = c * CORES + (core if w == 0 else 1 - core)
                src = xb.at[s, pl.ds(pl.multiple_of(to * t_loc, t_loc), t_loc)]
                pltpu.make_async_remote_copy(src_ref=src, dst_ref=dst.at[me], send_sem=y_send.at[s, hop * CORES + w],
                                             recv_sem=y_recv.at[s, hop * CORES + w], device_id={"sp": to}, device_id_type=MESH).start()

            for s_now in range(n_seq):
                @pl.when(jnp.logical_and(s == s_now, hop == 0))
                def _():
                    src = xb.at[s_now, pl.ds(pl.multiple_of(me * t_loc, t_loc), t_loc)]
                    pltpu.make_async_copy(src, y_outs[s_now].at[me], y_recv.at[s_now, 0]).start()
                    send(1, y_outs[s_now])

                @pl.when(jnp.logical_and(s == s_now, hop != 0))
                def _():
                    send(0, y_outs[s_now])
                    send(1, y_outs[s_now])
            return 0
        lax.fori_loop(0, chips, finish, 0)
        return 0

    lax.fori_loop(0, n_seq, sequence, 0)

    for s in range(n_seq):
        for tag in range(n):
            pltpu.make_async_copy(xb.at[s, pl.ds(0, t_loc)], y_outs[s].at[0], y_recv.at[s, tag]).wait()
    for s in range(n_seq):
        for tag in range(1, n):
            pltpu.make_async_copy(xb.at[s, pl.ds(0, t_loc)], y_outs[s].at[0], y_send.at[s, tag]).wait()
    for cp in sends:
        cp.wait_send()


def copy_kernel(early, last, dst, out_sem):
    others, n = early.shape[:2]
    writes = []
    for i in range(n):
        writes.append(pltpu.make_async_copy(last.at[i], dst.at[i * (others + 1) + others], out_sem.at[others, i]))
        for s in range(others):
            writes.append(pltpu.make_async_copy(early.at[s, i], dst.at[i * (others + 1) + s], out_sem.at[s, i]))
    for cp in writes:
        cp.start()
    for cp in writes:
        cp.wait()


def solution(mesh):
    n = mesh.shape["sp"]

    def local_block(x_loc, pos_loc, w_query, w_key, w_value, w_out, gain_q, gain_k, gain_out):
        batch, t_loc, width = x_loc.shape
        n_seq = batch // n
        inv_freq = 1.0 / (ROPE_THETA ** (np.arange(0, HEAD_DIM, 2, dtype=np.float32) / HEAD_DIM))
        freq = jnp.asarray(np.concatenate([inv_freq, inv_freq]).astype(np.float32)[None, :])
        hbm = pl.BlockSpec(memory_space=pl.ANY)
        seq = n * t_loc
        bf16 = jnp.bfloat16
        early, last = pl.pallas_call(
            functools.partial(block_kernel, n),
            out_shape=(pltpu.HBM((n_seq - 1, n, t_loc, width), bf16), pltpu.VMEM((n, t_loc, width), bf16)),
            in_specs=[hbm] * 10,
            out_specs=(hbm, hbm),
            scratch_shapes=[
                pltpu.VMEM((width, width), bf16), pltpu.VMEM((width, width), bf16), pltpu.VMEM((width, width), bf16), pltpu.VMEM((width, width), bf16),
                pltpu.VMEM((n_seq, seq, width), bf16),
                pltpu.VMEM((seq, width), bf16), pltpu.VMEM((seq, width), bf16), pltpu.VMEM((seq, width), bf16),
                pltpu.VMEM((CORES * t_loc, width), bf16),
                pltpu.VMEM((2, CORES * t_loc, seq), jnp.float32), pltpu.VMEM((2, CORES * t_loc, seq), bf16),
                pltpu.VMEM((1, HEAD_DIM), jnp.float32), pltpu.VMEM((width,), bf16), pltpu.VMEM((width,), bf16), pltpu.VMEM((width,), bf16),
                pltpu.VMEM((3, width), jnp.float32),
                pltpu.VMEM((n, batch, t_loc), jnp.int32),
                pltpu.VMEM((seq, HEAD_DIM), jnp.float32), pltpu.VMEM((seq, HEAD_DIM), jnp.float32),
                pltpu.SemaphoreType.DMA((4,)), pltpu.SemaphoreType.DMA((4,)),
                pltpu.SemaphoreType.DMA((n,)), pltpu.SemaphoreType.DMA((n,)),
                pltpu.SemaphoreType.DMA((n_seq, n)), pltpu.SemaphoreType.DMA((n_seq, n)),
                pltpu.SemaphoreType.DMA((n_seq, n)), pltpu.SemaphoreType.DMA((n_seq, n)),
            ],
            compiler_params=pltpu.CompilerParams(collective_id=0, has_side_effects=True, vmem_limit_bytes=VMEM_LIMIT - seq * width * 2),
            name="attention_block",
        )(x_loc, pos_loc, freq, gain_q, gain_k, gain_out, w_query, w_key, w_value, w_out)
        return pl.pallas_call(
            copy_kernel,
            out_shape=jax.ShapeDtypeStruct(x_loc.shape, bf16),
            in_specs=[pl.BlockSpec(memory_space=pltpu.VMEM), hbm],
            out_specs=hbm,
            scratch_shapes=[pltpu.SemaphoreType.DMA((n_seq, n))],
            compiler_params=pltpu.CompilerParams(vmem_limit_bytes=VMEM_LIMIT // 4),
            name="result_copy",
        )(early, last)

    tok_spec = P("dp", "sp", None)
    return jax.shard_map(local_block, mesh=mesh, in_specs=(tok_spec, P("dp", "sp"), P(), P(), P(), P(), P(), P(), P()), out_specs=tok_spec, check_vma=False)
```
